32 devices in a mesh: prow: 8 (over z, x), pcol: 4 (over y, core).
Axes of the slice: x: 2, y: 2, z: 4, core: 2. Of those that a mesh axis runs over, the one named last changes fastest.
Arguments:
- cross_cov: float32 [4, 8, 256, 8, 4, 256], P(None, 'prow', None, None, 'pcol'), may hold values from -6 to 6
- left_factor: float32 [4, 8, 256, 512], P(None, 'prow', None, 'pcol'), may hold values from -1 to 3, as said below
- right_factor: float32 [8, 4, 256, 512], P(None, 'pcol', None, 'prow'), may hold values from -1 to 3, as said below
Outputs:
- whitened: float32 [4, 8, 256, 8, 4, 256], P(None, 'prow', None, None, 'pcol')
The draws below stay inside these ranges and needn't reach their ends.
Inputs may be any that keep to these rules, and one draw needn't show every extreme that they name: `left_factor`: the diagonal entries of the diagonal blocks lie between 1.5 and 2. `right_factor`: the diagonal entries of the diagonal blocks lie between 1.5 and 2.
All inputs are finite; a program needn't handle non-finite values.
Results may differ from the reference program's by a relative error of at most 0.0001.
Values sent between devices are 32-bit elements; how exact they have to be, the bound alone decides.
A program may use at most 128 MiB of HBM per device.

```python
import math
import jax
import jax.numpy as jnp
from jax import lax

N = 8192
BS = 256
STEPS = 2
CYC_R = 4
CYC_C = 8
N_PROW = 8
N_PCOL = 4


def panel_draw(key, total_rows):
    first_key, second_key = jax.random.split(jax.random.fold_in(key, 11))
    columns = STEPS * BS
    base = jnp.clip(jax.random.normal(first_key, (total_rows, columns), jnp.float32), -3.0, 3.0) * 0.4
    base = base / math.sqrt(BS)
    diagonal = jax.random.uniform(second_key, (total_rows, 1), jnp.float32, 1.5, 2.0)
    row_ids = jnp.arange(total_rows)[:, None]
    col_ids = jnp.arange(columns)[None, :]
    return jnp.where(row_ids == col_ids, diagonal, base)


def draw_left_factor(key, part):
    return panel_draw(key, N).reshape(CYC_R, N_PROW, BS, STEPS * BS)


def draw_right_factor(key, part):
    return panel_draw(jax.random.fold_in(key, 5), N).reshape(CYC_C, N_PCOL, BS, STEPS * BS)


def steps_of(key, shape, cuts, low, high):
    def one(axis_at, shards_of):
        heights = jax.random.uniform(jax.random.fold_in(jax.random.fold_in(key, 6), axis_at), (shards_of,), jnp.float32, low / len(cuts), high / len(cuts))
        return jnp.repeat(jnp.exp(heights), shape[axis_at] // shards_of).reshape((-1,) + (1,) * (len(shape) - axis_at - 1))

    level = one(*cuts[0])
    for cut in cuts[1:]:
        level = level * one(*cut)
    return level


def noise(key, extent, deviation, most, shards=(), held_as=jnp.bfloat16):
    gain = steps_of(key, extent, shards, -0.22, 0.18) if shards else 1.0
    result = jax.random.normal(key, extent, jnp.float32) * deviation * gain
    return jnp.minimum(jnp.maximum(result, -most), most).astype(held_as)


def setup_inputs(seed: int = 0) -> dict:
    key_of = jax.random.split(jax.random.key(seed), 4)
    return {
        "cross_cov": noise(key_of[0], (CYC_R, N_PROW, BS, CYC_C, N_PCOL, BS), 1.0, 6.0, ((1, 8), (4, 4)), jnp.float32),
        "left_factor": draw_left_factor(jax.random.fold_in(key_of[3], 71), 0),
        "right_factor": draw_right_factor(jax.random.fold_in(key_of[3], 71), 0),
    }


def reference(cross_cov, left_factor, right_factor):
    whole = cross_cov.reshape(N, N)
    left_full = left_factor.reshape(N, STEPS * BS)
    right_full = right_factor.reshape(N, STEPS * BS)
    for block_step in range(STEPS):
        first_row = block_step * BS
        finish = first_row + BS
        solved = jax.scipy.linalg.solve_triangular(left_full[first_row:finish, first_row:finish], whole[first_row:finish], lower=True)
        lower_part = whole[finish:] - jnp.dot(left_full[finish:, first_row:finish], solved, precision=lax.Precision.HIGHEST)
        whole = jnp.concatenate([whole[:first_row], solved, lower_part], 0)
    for block_step in range(STEPS):
        first_col = block_step * BS
        finish = first_col + BS
        solved = jax.scipy.linalg.solve_triangular(right_full[first_col:finish, first_col:finish], whole[:, first_col:finish].T, lower=True).T
        right_part = whole[:, finish:] - jnp.dot(solved, right_full[finish:, first_col:finish].T, precision=lax.Precision.HIGHEST)
        whole = jnp.concatenate([whole[:, :first_col], solved, right_part], 1)
    return whole.reshape(cross_cov.shape)
```

```python
import functools

import jax
import jax.numpy as jnp
from jax import lax
from jax.experimental import pallas as pl
from jax.experimental.pallas import tpu as pltpu
from jax.sharding import PartitionSpec as P

STEPS = 2
CORES = 2
MESH = pl.DeviceIdType.MESH
HIGHEST = lax.Precision.HIGHEST
HIGH = lax.Precision.HIGH


def comm_kernel(nx, nprow, npcol, counts, st, lx, sl, ry, top, lyg, lxg, slg, stl, rtop, ltop, send_sem, recv_sem, local_sem):
    nz = nprow // nx
    ny = npcol // CORES
    cols = st.shape[0]
    prow = lax.axis_index("prow")
    pcol = lax.axis_index("pcol")
    z, x = lax.div(prow, nx), lax.rem(prow, nx)
    y, core = lax.div(pcol, CORES), lax.rem(pcol, CORES)
    x_others = [lax.rem(x + i, nx) for i in range(1, nx)]
    y_others = [lax.rem(y + i, ny) for i in range(1, ny)]
    sibling = {"pcol": y * CORES + (CORES - 1 - core)}
    up, down = {"prow": prow + nx}, {"prow": prow - nx}
    has_up, has_down = z < nz - 1, z > 0
    x_devices = [{"prow": z * nx + other} for other in x_others]
    y_devices = [{"pcol": other * CORES + core} for other in y_others]
    always = None

    def when(cond, action):
        if cond is None:
            action()
        else:
            pl.when(cond)(action)

    def both(first, second):
        if first is None:
            return second
        if second is None:
            return first
        return jnp.logical_and(first, second)

    barrier = pltpu.get_barrier_semaphore()
    for device, cond in [(up, has_up), (down, has_down)] + [(d, always) for d in x_devices + y_devices + [sibling]]:
        when(cond, lambda device=device: pl.semaphore_signal(barrier, inc=1, device_id=device, device_id_type=MESH))
    pl.semaphore_wait(barrier, nx - 1 + ny - 1 + 1 + has_up.astype(jnp.int32) + has_down.astype(jnp.int32))

    half = [(0, 1), (1, cols - 1)]
    pieces = len(half)
    base = [0]

    def region(count):
        first = base[0]
        base[0] += count
        return first

    ly_base, b_base, lt_base = region(nprow * pieces), region(STEPS * cols), region(STEPS)
    lx_base, ltg_base = region(npcol), region(npcol)
    sl_base, stl_base, rt_base = region(STEPS), region(STEPS), region(STEPS)
    counts["recv"] = base[0]

    def ly(p, j):
        return lyg.at[p, pl.ds(half[j][0], half[j][1])], ly_base + p * pieces + j

    def b(k, j):
        return top.at[k, j], b_base + k * cols + j

    def lt(k):
        return ltop.at[pcol, k], lt_base + k

    sends = []

    def send(item, devices, source=None):
        ref, rid = item
        for device, cond in devices:
            copy = pltpu.make_async_remote_copy(
                src_ref=ref if source is None else source,
                dst_ref=ref,
                send_sem=send_sem.at[len(sends)],
                recv_sem=recv_sem.at[rid],
                device_id=device,
                device_id_type=MESH,
            )
            sends.append((copy, cond))
            when(cond, copy.start)

    def receive(item, cond):
        ref, rid = item
        copy = pltpu.make_async_remote_copy(
            src_ref=ref, dst_ref=ref, send_sem=send_sem.at[0], recv_sem=recv_sem.at[rid], device_id=sibling, device_id_type=MESH
        )
        when(cond, copy.wait_recv)

    def to(devices, cond):
        return [(d, cond) for d in devices]

    lead = both(z == 0, x < STEPS if nx > STEPS else None)
    carries = both(z > 0, x < STEPS if nx > STEPS else None)
    owner_col = pcol < STEPS

    send(lt(x), [(up, lead)] + to(x_devices, lead), lx.at[0])
    send(b(x, 0), [(up, lead)] + to(x_devices, lead), st.at[0])
    for j in range(pieces):
        part = ry.at[pl.ds(half[j][0], half[j][1])]
        send(ly(prow, j), [(up, has_up), (down, has_down)] + to(x_devices, always), part)
        if j == 0:
            send((lxg.at[pcol], lx_base + pcol), to(y_devices + [sibling], always), lx)
            send((slg.at[pcol], sl_base + pcol), to(y_devices + [sibling], owner_col), sl)
    for j in range(1, cols):
        send(b(x, j), [(up, lead)] + to(x_devices, lead), st.at[j])
    locals_ = []

    def keep(source, ref, cond):
        copy = pltpu.make_async_copy(source, ref, local_sem.at[len(locals_)])
        locals_.append((copy, cond))
        when(cond, copy.start)

    keep(ry, lyg.at[prow], always)
    keep(lx, lxg.at[pcol], always)
    keep(sl, slg.at[pcol], owner_col)
    keep(st, top.at[prow], prow < STEPS)
    keep(lx.at[0], ltop.at[pcol, prow], prow < STEPS)

    def relay_up(item, cond):
        receive(item, cond)
        send(item, [(up, both(cond, has_up))] + to(x_devices, cond))

    def relay_down(item, cond):
        receive(item, cond)
        send(item, [(down, both(cond, has_down))] + to(x_devices, cond))

    def line(j):
        for piece in range(pieces):
            relay_up(ly((z - j) * nx + x, piece), z - j >= 1)
            relay_down(ly((z + j) * nx + x, piece), z + j <= nz - 1)

    if nz > 1:
        line(1)
    relay_up(lt(x), carries)
    relay_up(b(x, 0), carries)
    relay_up(ly(x, 0), z > 0)
    for j in range(2, nz):
        line(j)
        if j == 2:
            relay_up(ly(x, 1), z > 0)
    if nz <= 2:
        relay_up(ly(x, 1), z > 0)
    early = min(3, cols)
    for j in range(1, early):
        relay_up(b(x, j), carries)
    for other in y_others:
        item = (lxg.at[other * CORES + core], lx_base + other * CORES + core)
        receive(item, always)
        send(item, [(sibling, always)])
        from_owner = other * CORES + core < STEPS
        item = (slg.at[other * CORES + core], sl_base + other * CORES + core)
        receive(item, from_owner)
        send(item, [(sibling, from_owner)])
    for other in x_others:
        carried = other < STEPS if nx > STEPS else None
        receive(lt(other), carried)
        receive(b(other, 0), carried)
        for other_z in range(nz):
            receive(ly(other_z * nx + other, 0), always)
    for copy, cond in locals_:
        when(cond, copy.wait)
    send((ltop.at[pcol], ltg_base + pcol), to(y_devices + [sibling], always))
    send((stl.at[pcol], stl_base + pcol), to(y_devices + [sibling], owner_col), top.at[:, 0])
    send((rtop.at[pcol], rt_base + pcol), to(y_devices + [sibling], owner_col), lyg.at[:, 0])
    own = []
    for source, ref in ((top.at[:, 0], stl.at[pcol]), (lyg.at[:, 0], rtop.at[pcol])):
        copy = pltpu.make_async_copy(source, ref, local_sem.at[len(locals_) + len(own)])
        own.append(copy)
        when(owner_col, copy.start)
    for j in range(early, cols):
        relay_up(b(x, j), carries)
    for other in y_others:
        q = other * CORES + core
        item = (ltop.at[q], ltg_base + q)
        receive(item, always)
        send(item, [(sibling, always)])
        for ref, first in ((stl, stl_base), (rtop, rt_base)):
            item = (ref.at[q], first + q)
            receive(item, q < STEPS)
            send(item, [(sibling, q < STEPS)])
    for other_y in range(ny):
        q = other_y * CORES + (CORES - 1 - core)
        receive((lxg.at[q], lx_base + q), always)
        receive((ltop.at[q], ltg_base + q), always)
        for ref, first in ((slg, sl_base), (stl, stl_base), (rtop, rt_base)):
            receive((ref.at[q], first + q), q < STEPS)
    for other in x_others:
        carried = other < STEPS if nx > STEPS else None
        for other_z in range(nz):
            for piece in range(1, pieces):
                receive(ly(other_z * nx + other, piece), always)
        for j in range(1, cols):
            receive(b(other, j), carried)
    for copy in own:
        when(owner_col, copy.wait)
    for copy, cond in sends:
        when(cond, copy.wait_send)
    counts["send"] = len(sends)


def move(nx, st, lx, sl, ry):
    nprow, npcol = lax.axis_size("prow"), lax.axis_size("pcol")
    f32 = jnp.float32
    cols, size = st.shape[0], st.shape[1]
    shapes = [
        (STEPS,) + st.shape,
        (nprow,) + ry.shape,
        (npcol,) + lx.shape,
        (STEPS,) + sl.shape,
        (STEPS, STEPS, size, size),
        (STEPS, nprow) + ry.shape[1:],
        (npcol, STEPS) + lx.shape[1:],
    ]
    nz = nprow // nx
    receives = nprow * 2 + STEPS * cols + STEPS * 4 + npcol * 2
    fan = nx + npcol + 3
    sends = (cols + 4 + 2 * nz * 2 + cols + 8) * fan
    return pl.pallas_call(
        functools.partial(comm_kernel, nx, nprow, npcol, {}),
        out_shape=[jax.ShapeDtypeStruct(s, f32) for s in shapes],
        in_specs=[pl.BlockSpec(memory_space=pltpu.VMEM)] * 4,
        out_specs=[pl.BlockSpec(memory_space=pl.ANY)] * len(shapes),
        scratch_shapes=[
            pltpu.SemaphoreType.DMA((sends,)),
            pltpu.SemaphoreType.DMA((receives,)),
            pltpu.SemaphoreType.DMA((8,)),
        ],
        compiler_params=pltpu.CompilerParams(collective_id=0, has_side_effects=True),
    )(st, lx, sl, ry)


TILE = 128


def invert_kernel(in_ref, out_ref):
    count, order = in_ref.shape[0], in_ref.shape[1]
    tiles = order // TILE
    row = lax.broadcasted_iota(jnp.int32, (TILE, TILE), 0)
    col = lax.broadcasted_iota(jnp.int32, (TILE, TILE), 1)
    dot = functools.partial(jnp.dot, precision=HIGHEST, preferred_element_type=jnp.float32)
    out_ref[...] = jnp.zeros_like(out_ref)
    lows, invs = [], []
    for m in range(count):
        for t in range(tiles):
            low = in_ref[m, t * TILE : (t + 1) * TILE, t * TILE : (t + 1) * TILE]
            lows.append(low)
            invs.append(jnp.where(row == col, 1.0 / low, 0.0))
    span = 1
    while span < TILE:
        pick = jnp.logical_and(row // (2 * span) == col // (2 * span), jnp.logical_and(row // span % 2 == 1, col // span % 2 == 0))
        mids = [dot(jnp.where(pick, low, 0.0), inv) for low, inv in zip(lows, invs)]
        invs = [inv - dot(inv, mid) for mid, inv in zip(mids, invs)]
        span *= 2
    for m in range(count):
        for t in range(tiles):
            out_ref[m, t * TILE : (t + 1) * TILE, t * TILE : (t + 1) * TILE] = invs[m * tiles + t]
    span = TILE
    while span < order:
        for first in range(0, order, 2 * span):
            lo, mid, hi = first, first + span, first + 2 * span
            for m in range(count):
                inner = dot(in_ref[m, mid:hi, lo:mid], out_ref[m, lo:mid, lo:mid])
                out_ref[m, mid:hi, lo:mid] = -dot(out_ref[m, mid:hi, mid:hi], inner)
        span *= 2


def invert(lower):
    return pl.pallas_call(
        invert_kernel,
        out_shape=jax.ShapeDtypeStruct(lower.shape, lower.dtype),
        in_specs=[pl.BlockSpec(memory_space=pltpu.VMEM)],
        out_specs=pl.BlockSpec(memory_space=pltpu.VMEM),
    )(lower)


def shards(nx, cross_cov, left_factor, right_factor):
    nprow, npcol = lax.axis_size("prow"), lax.axis_size("pcol")
    prow, pcol = lax.axis_index("prow"), lax.axis_index("pcol")
    rows, _, size, cols, _, _ = cross_cov.shape
    depth = STEPS * size
    wide = depth // nprow
    fold = 128 // wide if wide < 128 else 1
    matrix = cross_cov.reshape(rows, size, cols, size)
    st = matrix[0].transpose(1, 0, 2)
    sl = matrix[:, :, 0]
    lx = left_factor[:, 0]
    ry = right_factor[:, 0].reshape(cols, fold, size // fold, wide).transpose(0, 2, 1, 3).reshape(cols, size // fold, fold * wide)
    top, lyg, lxg, slg, stl, rtop, ltop = move(nx, st, lx, sl, ry)

    def unfold(packed):
        groups = packed.shape[1]
        apart = packed.reshape(nprow, groups, size // fold, fold, wide)
        return apart.transpose(1, 3, 2, 0, 4).reshape(groups, size, depth)

    left_top = ltop.transpose(1, 2, 0, 3).reshape(depth, depth)
    right_top = unfold(rtop.transpose(1, 0, 2, 3)).reshape(depth, depth)
    left_inv, right_inv = invert(jnp.stack([left_top, right_top]))
    left = lxg.transpose(1, 2, 0, 3).reshape(rows, size, depth)
    right = unfold(lyg).reshape(cols, size, depth)

    def scaled(factor, inverse, index, axis_size):
        product = jnp.einsum("cij,jk->cik", factor, inverse, precision=HIGH)
        own = lax.dynamic_slice(inverse, (jnp.minimum(index, STEPS - 1) * size, 0), (size, depth))
        block = (jnp.arange(factor.shape[0]) * axis_size + index).reshape(-1, 1, 1)
        return jnp.where(block < STEPS, -own[None], product)

    w = scaled(left, left_inv, prow, nprow).reshape(rows * size, depth)
    v = scaled(right, right_inv, pcol, npcol).reshape(cols * size, depth)
    row_keep = (jnp.arange(rows) * nprow + prow >= STEPS).astype(jnp.float32)
    col_keep = (jnp.arange(cols) * npcol + pcol >= STEPS)
    corner = stl.transpose(1, 2, 0, 3).reshape(depth, depth)
    strip = slg.transpose(1, 2, 0, 3).reshape(rows, size, depth)
    strip = jnp.where(row_keep.reshape(-1, 1, 1) > 0, strip, 0.0).reshape(rows * size, depth)
    strip = strip - jnp.dot(w, corner, precision=HIGH)
    tops = jnp.where(col_keep.reshape(1, -1, 1, 1), top, 0.0).transpose(0, 2, 1, 3).reshape(depth, cols * size)
    a = jnp.concatenate([w, strip], 1)
    b = jnp.concatenate([tops, v.T], 0)
    update = jnp.dot(a, b, precision=HIGH).reshape(rows, size, cols, size)
    keep = (row_keep.reshape(-1, 1, 1, 1) > 0) & col_keep.reshape(1, 1, -1, 1)
    return (jnp.where(keep, matrix, 0.0) - update).reshape(cross_cov.shape)


def along_x(mesh):
    places = [getattr(d, "coords", None) for d in mesh.devices[:, 0]]
    if any(c is None for c in places):
        return STEPS
    return len({c[0] for c in places})


def solution(mesh):
    placed = (
        P(None, "prow", None, None, "pcol", None),
        P(None, "prow", None, "pcol"),
        P(None, "pcol", None, "prow"),
    )
    return jax.shard_map(
        functools.partial(shards, along_x(mesh)),
        mesh=mesh,
        in_specs=placed,
        out_specs=P(None, "prow", None, None, "pcol", None),
        check_vma=False,
    )
```

```python
import functools

import jax
import jax.numpy as jnp
from jax import lax
from jax.experimental import pallas as pl
from jax.experimental.pallas import tpu as pltpu
from jax.sharding import PartitionSpec as P

STEPS = 2
CORES = 2
MESH = pl.DeviceIdType.MESH
HIGHEST = lax.Precision.HIGHEST


def comm_kernel(nx, nprow, npcol, counts, st, lx, sl, ry, top, lyg, lxg, slg, stl, rtop, ltop, send_sem, recv_sem, local_sem):
    nz = nprow // nx
    ny = npcol // CORES
    cols = st.shape[0]
    prow = lax.axis_index("prow")
    pcol = lax.axis_index("pcol")
    z, x = lax.div(prow, nx), lax.rem(prow, nx)
    y, core = lax.div(pcol, CORES), lax.rem(pcol, CORES)
    x_others = [lax.rem(x + i, nx) for i in range(1, nx)]
    y_others = [lax.rem(y + i, ny) for i in range(1, ny)]
    sibling = {"pcol": y * CORES + (CORES - 1 - core)}
    up, down = {"prow": prow + nx}, {"prow": prow - nx}
    has_up, has_down = z < nz - 1, z > 0
    x_devices = [{"prow": z * nx + other} for other in x_others]
    y_devices = [{"pcol": other * CORES + core} for other in y_others]
    always = None

    def when(cond, action):
        if cond is None:
            action()
        else:
            pl.when(cond)(action)

    def both(first, second):
        if first is None:
            return second
        if second is None:
            return first
        return jnp.logical_and(first, second)

    barrier = pltpu.get_barrier_semaphore()
    for device, cond in [(up, has_up), (down, has_down)] + [(d, always) for d in x_devices + y_devices + [sibling]]:
        when(cond, lambda device=device: pl.semaphore_signal(barrier, inc=1, device_id=device, device_id_type=MESH))
    pl.semaphore_wait(barrier, nx - 1 + ny - 1 + 1 + has_up.astype(jnp.int32) + has_down.astype(jnp.int32))

    half = [(0, 1), (1, cols - 1)]
    pieces = len(half)
    base = [0]

    def region(count):
        first = base[0]
        base[0] += count
        return first

    ly_base, b_base, lt_base = region(nprow * pieces), region(STEPS * cols), region(STEPS)
    lx_base, ltg_base = region(npcol), region(npcol)
    sl_base, stl_base, rt_base = region(STEPS), region(STEPS), region(STEPS)
    counts["recv"] = base[0]

    def ly(p, j):
        return lyg.at[p, pl.ds(half[j][0], half[j][1])], ly_base + p * pieces + j

    def b(k, j):
        return top.at[k, j], b_base + k * cols + j

    def lt(k):
        return ltop.at[pcol, k], lt_base + k

    sends = []

    def send(item, devices, source=None):
        ref, rid = item
        for device, cond in devices:
            copy = pltpu.make_async_remote_copy(
                src_ref=ref if source is None else source,
                dst_ref=ref,
                send_sem=send_sem.at[len(sends)],
                recv_sem=recv_sem.at[rid],
                device_id=device,
                device_id_type=MESH,
            )
            sends.append((copy, cond))
            when(cond, copy.start)

    def receive(item, cond):
        ref, rid = item
        copy = pltpu.make_async_remote_copy(
            src_ref=ref, dst_ref=ref, send_sem=send_sem.at[0], recv_sem=recv_sem.at[rid], device_id=sibling, device_id_type=MESH
        )
        when(cond, copy.wait_recv)

    def to(devices, cond):
        return [(d, cond) for d in devices]

    lead = both(z == 0, x < STEPS if nx > STEPS else None)
    carries = both(z > 0, x < STEPS if nx > STEPS else None)
    owner_col = pcol < STEPS

    send(lt(x), [(up, lead)] + to(x_devices, lead), lx.at[0])
    send(b(x, 0), [(up, lead)] + to(x_devices, lead), st.at[0])
    for j in range(pieces):
        part = ry.at[pl.ds(half[j][0], half[j][1])]
        send(ly(prow, j), [(up, has_up), (down, has_down)] + to(x_devices, always), part)
        if j == 0:
            send((lxg.at[pcol], lx_base + pcol), to(y_devices + [sibling], always), lx)
            send((slg.at[pcol], sl_base + pcol), to(y_devices + [sibling], owner_col), sl)
    for j in range(1, cols):
        send(b(x, j), [(up, lead)], st.at[j])
    locals_ = []

    def keep(source, ref, cond):
        copy = pltpu.make_async_copy(source, ref, local_sem.at[len(locals_)])
        locals_.append((copy, cond))
        when(cond, copy.start)

    keep(ry, lyg.at[prow], always)
    keep(lx, lxg.at[pcol], always)
    keep(sl, slg.at[pcol], owner_col)
    keep(st, top.at[prow], prow < STEPS)
    keep(lx.at[0], ltop.at[pcol, prow], prow < STEPS)

    def relay_up(item, cond):
        receive(item, cond)
        send(item, [(up, both(cond, has_up))] + to(x_devices, cond))

    def relay_down(item, cond):
        receive(item, cond)
        send(item, [(down, both(cond, has_down))] + to(x_devices, cond))

    def line(j):
        for piece in range(pieces):
            relay_up(ly((z - j) * nx + x, piece), z - j >= 1)
            relay_down(ly((z + j) * nx + x, piece), z + j <= nz - 1)

    if nz > 1:
        line(1)
    relay_up(lt(x), carries)
    relay_up(b(x, 0), carries)
    relay_up(ly(x, 0), z > 0)
    for j in range(2, nz):
        line(j)
        if j == 2:
            relay_up(ly(x, 1), z > 0)
    if nz <= 2:
        relay_up(ly(x, 1), z > 0)
    for j in range(1, cols):
        send(b(x, j), to(x_devices, lead), st.at[j])
    early = min(6, cols)
    for j in range(1, early):
        relay_up(b(x, j), carries)
    for other in y_others:
        item = (lxg.at[other * CORES + core], lx_base + other * CORES + core)
        receive(item, always)
        send(item, [(sibling, always)])
        from_owner = other * CORES + core < STEPS
        item = (slg.at[other * CORES + core], sl_base + other * CORES + core)
        receive(item, from_owner)
        send(item, [(sibling, from_owner)])
    for other in x_others:
        carried = other < STEPS if nx > STEPS else None
        receive(lt(other), carried)
        receive(b(other, 0), carried)
        for other_z in range(nz):
            receive(ly(other_z * nx + other, 0), always)
    for copy, cond in locals_:
        when(cond, copy.wait)
    send((ltop.at[pcol], ltg_base + pcol), to(y_devices + [sibling], always))
    send((stl.at[pcol], stl_base + pcol), to(y_devices + [sibling], owner_col), top.at[:, 0])
    send((rtop.at[pcol], rt_base + pcol), to(y_devices + [sibling], owner_col), lyg.at[:, 0])
    own = []
    for source, ref in ((top.at[:, 0], stl.at[pcol]), (lyg.at[:, 0], rtop.at[pcol])):
        copy = pltpu.make_async_copy(source, ref, local_sem.at[len(locals_) + len(own)])
        own.append(copy)
        when(owner_col, copy.start)
    for j in range(early, cols):
        relay_up(b(x, j), carries)
    for other in y_others:
        q = other * CORES + core
        item = (ltop.at[q], ltg_base + q)
        receive(item, always)
        send(item, [(sibling, always)])
        for ref, first in ((stl, stl_base), (rtop, rt_base)):
            item = (ref.at[q], first + q)
            receive(item, q < STEPS)
            send(item, [(sibling, q < STEPS)])
    for other_y in range(ny):
        q = other_y * CORES + (CORES - 1 - core)
        receive((lxg.at[q], lx_base + q), always)
        receive((ltop.at[q], ltg_base + q), always)
        for ref, first in ((slg, sl_base), (stl, stl_base), (rtop, rt_base)):
            receive((ref.at[q], first + q), q < STEPS)
    for other in x_others:
        carried = other < STEPS if nx > STEPS else None
        for other_z in range(nz):
            for piece in range(1, pieces):
                receive(ly(other_z * nx + other, piece), always)
        for j in range(1, cols):
            receive(b(other, j), carried)
    for copy in own:
        when(owner_col, copy.wait)
    for copy, cond in sends:
        when(cond, copy.wait_send)
    counts["send"] = len(sends)


def move(nx, st, lx, sl, ry):
    nprow, npcol = lax.axis_size("prow"), lax.axis_size("pcol")
    f32 = jnp.float32
    cols, size = st.shape[0], st.shape[1]
    shapes = [
        (STEPS,) + st.shape,
        (nprow,) + ry.shape,
        (npcol,) + lx.shape,
        (STEPS,) + sl.shape,
        (STEPS, STEPS, size, size),
        (STEPS, nprow) + ry.shape[1:],
        (npcol, STEPS) + lx.shape[1:],
    ]
    nz = nprow // nx
    receives = nprow * 2 + STEPS * cols + STEPS * 4 + npcol * 2
    fan = nx + npcol + 3
    sends = (cols + 4 + 2 * nz * 2 + cols + 8) * fan
    return pl.pallas_call(
        functools.partial(comm_kernel, nx, nprow, npcol, {}),
        out_shape=[jax.ShapeDtypeStruct(s, f32) for s in shapes],
        in_specs=[pl.BlockSpec(memory_space=pltpu.VMEM)] * 4,
        out_specs=[pl.BlockSpec(memory_space=pl.ANY)] * len(shapes),
        scratch_shapes=[
            pltpu.SemaphoreType.DMA((sends,)),
            pltpu.SemaphoreType.DMA((receives,)),
            pltpu.SemaphoreType.DMA((8,)),
        ],
        compiler_params=pltpu.CompilerParams(collective_id=0, has_side_effects=True),
    )(st, lx, sl, ry)


TILE = 128


def halves(x):
    high = x.astype(jnp.bfloat16)
    return high, (x - high.astype(jnp.float32)).astype(jnp.bfloat16)


def dot3(a, b, dims):
    (ah, al), (bh, bl) = a, b
    go = functools.partial(lax.dot_general, dimension_numbers=(dims, ((), ())), preferred_element_type=jnp.float32)
    return go(ah, bh) + (go(ah, bl) + go(al, bh))


NN = ((1,), (0,))
NT = ((1,), (1,))


def invert(low_ref, inv_ref):
    count, order = low_ref.shape[0], low_ref.shape[1]
    tiles = order // TILE
    row = lax.broadcasted_iota(jnp.int32, (TILE, TILE), 0)
    col = lax.broadcasted_iota(jnp.int32, (TILE, TILE), 1)
    dot = functools.partial(jnp.dot, precision=HIGHEST, preferred_element_type=jnp.float32)
    inv_ref[...] = jnp.zeros_like(inv_ref)
    lows, invs = [], []
    for m in range(count):
        for t in range(tiles):
            low = low_ref[m, t * TILE : (t + 1) * TILE, t * TILE : (t + 1) * TILE]
            lows.append(low)
            invs.append(jnp.where(row == col, 1.0 / low, 0.0))
    span = 1
    while span < TILE:
        pick = jnp.logical_and(row // (2 * span) == col // (2 * span), jnp.logical_and(row // span % 2 == 1, col // span % 2 == 0))
        mids = [dot(jnp.where(pick, low, 0.0), inv) for low, inv in zip(lows, invs)]
        invs = [inv - dot(inv, mid) for mid, inv in zip(mids, invs)]
        span *= 2
    for m in range(count):
        for t in range(tiles):
            inv_ref[m, t * TILE : (t + 1) * TILE, t * TILE : (t + 1) * TILE] = invs[m * tiles + t]
    span = TILE
    while span < order:
        for first in range(0, order, 2 * span):
            lo, mid, hi = first, first + span, first + 2 * span
            for m in range(count):
                inner = dot(low_ref[m, mid:hi, lo:mid], inv_ref[m, lo:mid, lo:mid])
                inv_ref[m, mid:hi, lo:mid] = -dot(inv_ref[m, mid:hi, mid:hi], inner)
        span *= 2


def unfolded(pieces, fold):
    wide = pieces[0].shape[1] // fold
    return jnp.concatenate(
        [jnp.concatenate([piece[:, h * wide : (h + 1) * wide] for piece in pieces], 1) for h in range(fold)], 0
    )


def finish_kernel(nprow, npcol, fold, m_ref, top_ref, lyg_ref, lxg_ref, slg_ref, stl_ref, rtop_ref, ltop_ref, out_ref, low_ref, inv_ref, w_ref, s_ref, r_ref):
    size = m_ref.shape[2]
    total = m_ref.shape[1]
    depth = STEPS * size
    prow, pcol = lax.axis_index("prow"), lax.axis_index("pcol")
    step = pl.program_id(0)

    @pl.when(step == 0)
    def _():
        for k in range(STEPS):
            span = slice(k * size, (k + 1) * size)
            low_ref[0, span, :] = jnp.concatenate([ltop_ref[q, k] for q in range(npcol)], 1)
            low_ref[1, span, :] = unfolded([rtop_ref[k, p] for p in range(nprow)], fold)
        invert(low_ref, inv_ref)
        left_inv = halves(inv_ref[0])
        r_ref[0], r_ref[1] = halves(inv_ref[1])
        left = jnp.concatenate([lxg_ref[q].reshape(total, depth // npcol) for q in range(npcol)], 1)
        w = dot3(halves(left), left_inv, NN)
        own = inv_ref[0, pl.ds(pl.multiple_of(jnp.minimum(prow, STEPS - 1) * size, size), size), :]
        w_high, w_low = halves(w)
        w_ref[0], w_ref[1] = w_high, w_low

        @pl.when(prow < STEPS)
        def _():
            own_high, own_low = halves(-own)
            w_ref[0, :size], w_ref[1, :size] = own_high, own_low

        corner = jnp.concatenate([jnp.concatenate([stl_ref[k, b] for b in range(STEPS)], 0) for k in range(STEPS)], 1)
        strip = jnp.concatenate([slg_ref[k].reshape(total, size) for k in range(STEPS)], 1)
        row = lax.broadcasted_iota(jnp.int32, strip.shape, 0)
        strip = jnp.where(jnp.logical_and(row < size, prow < STEPS), 0.0, strip)
        strip = strip - dot3((w_ref[0], w_ref[1]), halves(corner), NN)
        s_ref[0], s_ref[1] = halves(strip)

    solved_col = jnp.logical_and(step == 0, pcol < STEPS)
    right = unfolded([lyg_ref[p, 0] for p in range(nprow)], fold)
    v = dot3(halves(right), (r_ref[0], r_ref[1]), NN)
    own = inv_ref[1, pl.ds(pl.multiple_of(jnp.minimum(pcol, STEPS - 1) * size, size), size), :]
    v = jnp.where(solved_col, -own, v)
    tops = jnp.concatenate([top_ref[k, 0] for k in range(STEPS)], 0)
    tops = jnp.where(solved_col, 0.0, tops)
    update = dot3((w_ref[0], w_ref[1]), halves(tops), NN) + dot3((s_ref[0], s_ref[1]), halves(v), NT)
    row = lax.broadcasted_iota(jnp.int32, (total, size), 0)
    gone = jnp.logical_or(solved_col, jnp.logical_and(row < size, prow < STEPS))
    out_ref[0] = jnp.where(gone, 0.0, m_ref[0]) - update


def finish(fold, m, top, lyg, lxg, slg, stl, rtop, ltop):
    nprow, npcol = lax.axis_size("prow"), lax.axis_size("pcol")
    cols, total, size = m.shape
    depth = STEPS * size

    def whole(x):
        return pl.BlockSpec(x.shape, lambda d: (0,) * x.ndim)

    block = pl.BlockSpec((1, total, size), lambda d: (d, 0, 0))
    return pl.pallas_call(
        functools.partial(finish_kernel, nprow, npcol, fold),
        grid=(cols,),
        out_shape=jax.ShapeDtypeStruct(m.shape, m.dtype),
        in_specs=[
            block,
            pl.BlockSpec((STEPS, 1, size, size), lambda d: (0, d, 0, 0)),
            pl.BlockSpec((nprow, 1) + lyg.shape[2:], lambda d: (0, d, 0, 0)),
        ]
        + [whole(x) for x in (lxg, slg, stl, rtop, ltop)],
        out_specs=block,
        scratch_shapes=[
            pltpu.VMEM((2, depth, depth), jnp.float32),
            pltpu.VMEM((2, depth, depth), jnp.float32),
            pltpu.VMEM((2, total, depth), jnp.bfloat16),
            pltpu.VMEM((2, total, depth), jnp.bfloat16),
            pltpu.VMEM((2, depth, depth), jnp.bfloat16),
        ],
        compiler_params=pltpu.CompilerParams(dimension_semantics=("arbitrary",), vmem_limit_bytes=56 * 1024 * 1024),
    )(m, top, lyg, lxg, slg, stl, rtop, ltop)


def shards(nx, cross_cov, left_factor, right_factor):
    nprow = lax.axis_size("prow")
    rows, _, size, cols, _, _ = cross_cov.shape
    wide = STEPS * size // nprow
    fold = TILE // wide if wide < TILE else 1
    m = cross_cov.transpose(3, 0, 1, 2, 4, 5).reshape(cols, rows * size, size)
    st = m[:, :size]
    sl = m[0].reshape(rows, size, size)
    lx = left_factor[:, 0]
    ry = right_factor[:, 0].reshape(cols, fold, size // fold, wide).transpose(0, 2, 1, 3).reshape(cols, size // fold, fold * wide)
    moved = move(nx, st, lx, sl, ry)
    out = finish(fold, m, *moved)
    return out.reshape(cols, rows, 1, size, 1, size).transpose(1, 2, 3, 0, 4, 5)


def along_x(mesh):
    places = [getattr(d, "coords", None) for d in mesh.devices[:, 0]]
    if any(c is None for c in places):
        return STEPS
    return len({c[0] for c in places})


def solution(mesh):
    placed = (
        P(None, "prow", None, None, "pcol", None),
        P(None, "prow", None, "pcol"),
        P(None, "pcol", None, "prow"),
    )
    return jax.shard_map(
        functools.partial(shards, along_x(mesh)),
        mesh=mesh,
        in_specs=placed,
        out_specs=P(None, "prow", None, None, "pcol", None),
        check_vma=False,
    )
```
